32 devices in a mesh: dp: 8 (over z, core), seq: 4 (over y, x).
Axes of the slice: x: 2, y: 2, z: 4, core: 2. Of those that a mesh axis runs over, the one named last changes fastest.
Arguments:
- tokens: bfloat16 [32, 256, 1024], P(('dp', 'seq')), may hold values from -6 to 6
- queries: bfloat16 [32, 256, 1024], P(('dp', 'seq')), may hold values from -240 to 240
- keys: bfloat16 [32, 256, 1024], P(('dp', 'seq')), may hold values from -7 to 7
- values: bfloat16 [32, 256, 1024], P(('dp', 'seq')), may hold values from -6 to 6
- ln_gain: bfloat16 [1024], replicated, may hold values from 0.5 to 1.5
- mean_in: bfloat16 [1024, 2048], P(None, 'seq'), may hold values from -0.1875 to 0.1875
- sigma_in: bfloat16 [1024, 2048], P(None, 'seq'), may hold values from 0.0039978027 to 0.029907227
- noise_in: bfloat16 [1024, 2048], P(None, 'seq'), may hold values from -4 to 4
- mean_out: bfloat16 [2048, 1024], P('seq'), may hold values from -0.125 to 0.125
- sigma_out: bfloat16 [2048, 1024], P('seq'), may hold values from 0.0019989014 to 0.014953613
- noise_out: bfloat16 [2048, 1024], P('seq'), may hold values from -4 to 4
- flip_in: int32 [32, 1024], P('dp'), may hold values from -1 to 1, as said below
- flip_mid: int32 [32, 2048], P('dp', 'seq'), may hold values from -1 to 1, as said below
- flip_hidden: int32 [32, 2048], P('dp', 'seq'), may hold values from -1 to 1, as said below
- flip_out: int32 [32, 1024], P('dp'), may hold values from -1 to 1, as said below
- cotangent: bfloat16 [32, 256, 1024], P(('dp', 'seq')), may hold values from -0.75 to 0.75
Outputs:
- block_out: bfloat16 [32, 256, 1024], P(('dp', 'seq'))
- resid_grad: bfloat16 [32, 256, 1024], P(('dp', 'seq'))
- grad_mean_in: float32 [1024, 2048], P(None, 'seq')
- grad_sigma_in: float32 [1024, 2048], P(None, 'seq')
- grad_mean_out: float32 [2048, 1024], P('seq')
- grad_sigma_out: float32 [2048, 1024], P('seq')
The draws below stay inside these ranges and needn't reach their ends.
Inputs may be any that keep to these rules, and one draw needn't show every extreme that they name: `flip_in`: each entry is -1 or +1. `flip_mid`: each entry is -1 or +1. `flip_hidden`: each entry is -1 or +1. `flip_out`: each entry is -1 or +1.
All inputs are finite; a program needn't handle non-finite values.
Results may differ from the reference program's by a relative error of at most 0.018.
Values may be sent and summed in bfloat16 or wider, within the bound.
A program may use at most 128 MiB of HBM per device.

```python
import math
import jax
import jax.numpy as jnp
from jax import lax

D = 1024
HEADS = 16
FF = 2048
PATCH = 256
IMAGES = 32
N_SEQ = 4


def query_key_pair(key):
    base = jax.random.fold_in(key, 4242)
    key_q, key_k = jax.random.split(base, 2)
    queries = jnp.clip(jax.random.normal(key_q, (IMAGES, PATCH, D), jnp.float32), -6.0, 6.0)
    keys = jnp.clip(jax.random.normal(key_k, (IMAGES, PATCH, D), jnp.float32), -6.0, 6.0)
    return (queries, keys)


def draw_queries(key, part):
    return query_key_pair(key)[0].astype(jnp.bfloat16)


def draw_keys(key, part):
    return query_key_pair(key)[1].astype(jnp.bfloat16)


def sign_table(key, salt, rows, cols):
    bits = jax.random.randint(jax.random.fold_in(key, salt), (rows, cols), 0, 2, jnp.int32)
    return 2 * bits - 1


def draw_flip_in(key, part):
    return sign_table(key, 11, IMAGES, D)


def draw_flip_mid(key, part):
    return sign_table(key, 23, IMAGES, FF)


def draw_flip_hidden(key, part):
    return sign_table(key, 37, IMAGES, FF)


def draw_flip_out(key, part):
    return sign_table(key, 53, IMAGES, D)


def levels(rng, extent, cuts, least, top_value):
    def one(dim, parts):
        heights = jax.random.uniform(jax.random.fold_in(jax.random.fold_in(rng, 6), dim), (parts,), jnp.float32, least / len(cuts), top_value / len(cuts))
        return jnp.repeat(jnp.exp(heights), extent[dim] // parts).reshape((-1,) + (1,) * (len(extent) - dim - 1))

    loudness = one(*cuts[0])
    for cut in cuts[1:]:
        loudness = loudness * one(*cut)
    return loudness


def gaussian(stream_key, extent, width, most, shards=(), kind=jnp.bfloat16):
    result = width * jax.random.normal(stream_key, extent, jnp.float32)
    if shards:
        result = result * levels(stream_key, extent, shards, -0.22, 0.18)
    return jnp.clip(result, -most, most).astype(kind)


def setup_inputs(seed: int = 0) -> dict:
    arg_keys = jax.random.split(jax.random.key(seed), 17)
    return {
        "tokens": gaussian(arg_keys[0], (IMAGES, PATCH, D), 1.0, 6.0, ((0, 32),)),
        "queries": draw_queries(jax.random.fold_in(arg_keys[16], 71), 0),
        "keys": draw_keys(jax.random.fold_in(arg_keys[16], 71), 0),
        "values": gaussian(arg_keys[3], (IMAGES, PATCH, D), 1.0, 6.0, ((0, 32),)),
        "ln_gain": jnp.clip(1.0 + 0.1 * jax.random.normal(arg_keys[4], (D,), jnp.float32), 0.5, 1.5).astype(jnp.bfloat16),
        "mean_in": gaussian(arg_keys[5], (D, FF), D ** -0.5, 0.1875, ((1, 4),)),
        "sigma_in": jnp.clip(jnp.exp(math.log(0.029907227) - 2.01235525 * jax.random.uniform(arg_keys[6], (D, FF), jnp.float32) ** levels(arg_keys[6], (D, FF), ((1, 4),), -0.2, 0.2)), 0.0039978027, 0.029907227).astype(jnp.bfloat16),
        "noise_in": gaussian(arg_keys[7], (D, FF), 1.0, 4.0, ((1, 4),)),
        "mean_out": gaussian(arg_keys[8], (FF, D), FF ** -0.5, 0.125, ((0, 4),)),
        "sigma_out": jnp.clip(jnp.exp(math.log(0.014953613) - 2.01235525 * jax.random.uniform(arg_keys[9], (FF, D), jnp.float32) ** levels(arg_keys[9], (FF, D), ((0, 4),), -0.2, 0.2)), 0.0019989014, 0.014953613).astype(jnp.bfloat16),
        "noise_out": gaussian(arg_keys[10], (FF, D), 1.0, 4.0, ((0, 4),)),
        "flip_in": draw_flip_in(jax.random.fold_in(arg_keys[16], 71), 0),
        "flip_mid": draw_flip_mid(jax.random.fold_in(arg_keys[16], 71), 0),
        "flip_hidden": draw_flip_hidden(jax.random.fold_in(arg_keys[16], 71), 0),
        "flip_out": draw_flip_out(jax.random.fold_in(arg_keys[16], 71), 0),
        "cotangent": gaussian(arg_keys[15], (IMAGES, PATCH, D), 0.125, 0.75, ((0, 32),)),
    }


def attend(query_img, key_img, value_img):
    head_dim = D // HEADS
    qf = query_img.astype(jnp.float32).reshape(PATCH, HEADS, head_dim)
    kf = key_img.astype(jnp.float32).reshape(PATCH, HEADS, head_dim)
    vf = value_img.astype(jnp.float32).reshape(PATCH, HEADS, head_dim)
    scores = jnp.einsum('qhe,khe->hqk', qf, kf) * head_dim ** (-0.5)
    top = lax.optimization_barrier(jnp.max(scores, axis=-1, keepdims=True))
    expd = jnp.exp(scores - top)
    total = lax.optimization_barrier(jnp.sum(expd, axis=-1))
    weights = expd.astype(jnp.bfloat16).astype(jnp.float32)
    outs = jnp.einsum('hqk,khe->qhe', weights, vf) / jnp.transpose(total)[:, :, None]
    return outs.reshape(PATCH, D).astype(jnp.bfloat16)

def gelu_slope(pre):
    cdf = 0.5 * (1.0 + lax.erf(pre * 0.7071067811865476))
    pdf = jnp.exp(-0.5 * pre * pre) * 0.3989422804014327
    return cdf + pre * pdf

def contract_first(left, right):
    return lax.dot_general(left, right, (((0,), (0,)), ((), ())), preferred_element_type=jnp.float32)

def contract_last(left, right):
    return lax.dot_general(left, right, (((1,), (1,)), ((), ())), preferred_element_type=jnp.float32)

def reference(tokens, queries, keys, values, ln_gain, mean_in, sigma_in, noise_in, mean_out, sigma_out, noise_out, flip_in, flip_mid, flip_hidden, flip_out, cotangent):
    bf = jnp.bfloat16
    f32 = jnp.float32
    attn_out = lax.map(lambda trio: attend(trio[0], trio[1], trio[2]), (queries, keys, values))
    resid = (tokens.astype(f32) + attn_out.astype(f32)).astype(bf)
    resid_f = resid.astype(f32)
    centered = resid_f - lax.optimization_barrier(jnp.mean(resid_f, axis=-1, keepdims=True))
    rstd = lax.rsqrt(lax.optimization_barrier(jnp.mean(centered * centered, axis=-1, keepdims=True)) + 1e-06)
    ahat = centered * rstd
    gain_f = ln_gain.astype(f32)
    normed = (ahat * gain_f).astype(bf)
    pert_in = (sigma_in.astype(f32) * noise_in.astype(f32)).astype(bf)
    pert_out = (sigma_out.astype(f32) * noise_out.astype(f32)).astype(bf)
    in_signs = flip_in.astype(bf)[:, None, :]
    mid_signs = flip_mid.astype(f32)[:, None, :]
    hid_signs = flip_hidden.astype(bf)[:, None, :]
    out_signs = flip_out.astype(f32)[:, None, :]
    rows = PATCH * IMAGES
    flat = normed.reshape(rows, D)
    flat_flip = (normed * in_signs).reshape(rows, D)
    pre = jnp.dot(flat, mean_in, preferred_element_type=f32).reshape(IMAGES, PATCH, FF)
    pre = pre + jnp.dot(flat_flip, pert_in, preferred_element_type=f32).reshape(IMAGES, PATCH, FF) * mid_signs
    hidden = jax.nn.gelu(pre, approximate=False).astype(bf)
    flipped_hidden = hidden * hid_signs
    block = FF // N_SEQ
    mixed = jnp.zeros((IMAGES, PATCH, D), f32)
    for index in range(N_SEQ):
        lo = index * block
        hb = hidden[:, :, lo:lo + block].reshape(rows, block)
        hfb = flipped_hidden[:, :, lo:lo + block].reshape(rows, block)
        part = jnp.dot(hb, mean_out[lo:lo + block], preferred_element_type=f32).reshape(IMAGES, PATCH, D)
        part = part + jnp.dot(hfb, pert_out[lo:lo + block], preferred_element_type=f32).reshape(IMAGES, PATCH, D) * out_signs
        mixed = mixed + part.astype(bf).astype(f32)
    block_out = (resid_f + mixed).astype(bf)
    cot_flip = cotangent * flip_out.astype(bf)[:, None, :]
    cot_flat = cotangent.reshape(rows, D)
    cot_flip_flat = cot_flip.reshape(rows, D)
    dhidden = contract_last(cot_flat, mean_out).reshape(IMAGES, PATCH, FF)
    dhidden = dhidden + contract_last(cot_flip_flat, pert_out).reshape(IMAGES, PATCH, FF) * flip_hidden.astype(f32)[:, None, :]
    dpre = (dhidden * gelu_slope(pre)).astype(bf)
    dpre_flip = dpre * flip_mid.astype(bf)[:, None, :]
    grad_mean_out = contract_first(hidden.reshape(rows, FF), cot_flat)
    grad_sigma_out = contract_first(flipped_hidden.reshape(rows, FF), cot_flip_flat) * noise_out.astype(f32)
    grad_mean_in = contract_first(flat, dpre.reshape(rows, FF))
    grad_sigma_in = contract_first(flat_flip, dpre_flip.reshape(rows, FF)) * noise_in.astype(f32)
    dnormed = jnp.zeros((IMAGES, PATCH, D), f32)
    in_signs_f = flip_in.astype(f32)[:, None, :]
    for index in range(N_SEQ):
        lo = index * block
        db = dpre[:, :, lo:lo + block].reshape(rows, block)
        dfb = dpre_flip[:, :, lo:lo + block].reshape(rows, block)
        part = contract_last(db, mean_in[:, lo:lo + block]).reshape(IMAGES, PATCH, D)
        part = part + contract_last(dfb, pert_in[:, lo:lo + block]).reshape(IMAGES, PATCH, D) * in_signs_f
        dnormed = dnormed + part.astype(bf).astype(f32)
    scaled = dnormed * gain_f
    back = rstd * (scaled - lax.optimization_barrier(jnp.mean(scaled, axis=-1, keepdims=True)) - ahat * lax.optimization_barrier(jnp.mean(scaled * ahat, axis=-1, keepdims=True)))
    resid_grad = (cotangent.astype(f32) + back).astype(bf)
    return (block_out, resid_grad, grad_mean_in, grad_sigma_in, grad_mean_out, grad_sigma_out)
```

```python
import functools
import math

import jax
import jax.numpy as jnp
from jax import lax
from jax.experimental import pallas as pl
from jax.experimental.pallas import tpu as pltpu
from jax.sharding import PartitionSpec as P

HEADS = 16
LANES = 128
CORES = 2
BF = jnp.bfloat16
F32 = jnp.float32
MESH = pl.DeviceIdType.MESH


def piece_shape(rows, cols, dp):
    if (rows // dp) % 16 == 0:
        return rows // dp, cols
    return rows * CORES // dp, cols // CORES


def dot_last(left, right):
    return lax.dot_general(left, right, (((1,), (1,)), ((), ())), preferred_element_type=F32)


def dot_first(left, right):
    return lax.dot_general(left, right, (((0,), (0,)), ((), ())), preferred_element_type=F32)


def dot(left, right):
    return jnp.dot(left, right, preferred_element_type=F32)


def norm_stats(resid_f):
    centered = resid_f - jnp.mean(resid_f, axis=-1, keepdims=True)
    rstd = lax.rsqrt(jnp.mean(centered * centered, axis=-1, keepdims=True) + 1e-06)
    return centered * rstd, rstd


def kernel(
    dp,
    seq,
    tok, que, key, val, gain, mean_in, sig_in, noi_in, mean_out, sig_out, noi_out,
    f_in, f_mid, f_hid, f_out, cot,
    out_block, out_grad, o_mo, o_so, o_mi, o_si,
    pert_in, pert_out, resid, cot_all, nrm_all, hid, hid_f, dpre, dpre_f,
    own, part_m, part_d, got_m, got_d,
    pieces, pairs, ups, downs, fulls,
    cot_s, cot_r, nrm_s, nrm_r, mix_s, mix_r, dnr_s, dnr_r,
    pair_s, pair_r, up_s, up_r, dn_s, dn_r, gu_s, gu_r, gd_s, gd_r, gp_s, gp_r, out_sem,
):
    my_dp = lax.axis_index("dp")
    me = lax.axis_index("seq")
    nz = dp // CORES
    z = my_dp // CORES
    core = my_dp % CORES
    partner = (z * CORES + (1 - core), me)
    above = (my_dp + CORES, me)
    below = (my_dp - CORES, me)
    base = math.isqrt(seq)
    if base * base != seq:
        base = seq
    tall = seq // base
    slots = part_m.shape[0]
    patches, width = resid.shape
    head_dim = width // HEADS
    scale = head_dim ** (-0.5)

    def shifted(k, sign):
        row = (me // base + sign * (k // base) + tall) % tall
        return row * base + (me % base + sign * (k % base) + base) % base

    def remote(src, dst, s, r, dev):
        return pltpu.make_async_remote_copy(
            src_ref=src, dst_ref=dst, send_sem=s, recv_sem=r, device_id=dev, device_id_type=MESH
        )

    def peer(index):
        return (my_dp, index)

    barrier = pltpu.get_barrier_semaphore()

    def greet(dev):
        pl.semaphore_signal(barrier, inc=1, device_id=dev, device_id_type=MESH)

    for k in range(1, seq):
        greet(peer(shifted(k, 1)))
    greet(partner)

    @pl.when(z > 0)
    def _():
        greet(below)

    @pl.when(z < nz - 1)
    def _():
        greet(above)

    chained = (z + nz - 1) // nz + (nz - 1 - z + nz - 1) // nz
    pl.semaphore_wait(barrier, seq + chained)

    def cot_copy(k):
        return remote(cot.at[0], cot_all.at[me], cot_s.at[k], cot_r.at[me], peer(shifted(k, 1)))

    def nrm_copy(k):
        return remote(
            nrm_all.at[me], nrm_all.at[me], nrm_s.at[k], nrm_r.at[me], peer(shifted(k, 1))
        )

    for k in range(1, seq):
        cot_copy(k).start()

    group = LANES // head_dim
    lane = lax.broadcasted_iota(jnp.int32, (1, LANES), 1)
    masks = [
        jnp.where((lane >= h * head_dim) & (lane < (h + 1) * head_dim), 1.0, 0.0).astype(F32)
        for h in range(group)
    ]

    def heads(p, carry):
        cols = pl.ds(pl.multiple_of(p * LANES, LANES), LANES)
        q, kk, v = que[0, :, cols], key[0, :, cols], val[0, :, cols]
        acc = jnp.zeros((patches, LANES), F32)
        for mask in masks:
            scores = dot_last(q * mask.astype(BF), kk) * scale
            expd = jnp.exp(scores - jnp.max(scores, axis=-1, keepdims=True))
            total = jnp.sum(expd, axis=-1, keepdims=True)
            acc = acc + (dot(expd.astype(BF), v) / total) * mask
        attn = acc.astype(BF).astype(F32)
        resid[:, cols] = (tok[0, :, cols].astype(F32) + attn).astype(BF)
        return carry

    lax.fori_loop(0, width // LANES, heads, 0)
    gain_f = gain[...].astype(F32)
    ahat, _ = norm_stats(resid[...].astype(F32))
    nrm_all[me] = (ahat * gain_f).astype(BF)
    for k in range(1, seq):
        nrm_copy(k).start()

    pert_in[...] = (sig_in[...].astype(F32) * noi_in[...].astype(F32)).astype(BF)
    pert_out[...] = (sig_out[...].astype(F32) * noi_out[...].astype(F32)).astype(BF)
    cot_all[me] = cot[0]

    def mix_copy(k, j):
        slot = (k - 1) % slots
        return remote(part_m.at[slot], got_m.at[me], mix_s.at[slot], mix_r.at[me], peer(j))

    def dnr_copy(k, j):
        slot = (k - 1) % slots
        return remote(part_d.at[slot], got_d.at[me], dnr_s.at[slot], dnr_r.at[me], peer(j))

    def arrived(dst, sem):
        remote(dst, dst, sem, sem, peer(me)).wait_recv()

    def signs(ref, j):
        return ref[pl.ds(j, 1), :].astype(F32)

    def block(k, first):
        j = me if first else shifted(k, -1)
        s_in, s_mid, s_hid, s_out = signs(f_in, j), signs(f_mid, j), signs(f_hid, j), signs(f_out, j)
        if not first:
            arrived(nrm_all.at[j], nrm_r.at[j])
        x = nrm_all[j]
        pre = dot(x, mean_in[...]) + dot(x * s_in.astype(BF), pert_in[...]) * s_mid
        cdf = 0.5 * (1.0 + lax.erf(pre * 0.7071067811865476))
        slope = cdf + pre * (jnp.exp(-0.5 * pre * pre) * 0.3989422804014327)
        h = (pre * cdf).astype(BF)
        hf = h * s_hid.astype(BF)
        hid[j] = h
        hid_f[j] = hf
        mixed = (dot(h, mean_out[...]) + dot(hf, pert_out[...]) * s_out).astype(BF)
        if first:
            own[0] = mixed
        else:
            @pl.when(k > slots)
            def _():
                mix_copy(k, j).wait_send()
                dnr_copy(k, j).wait_send()

            part_m[(k - 1) % slots] = mixed
            mix_copy(k, j).start()
            arrived(cot_all.at[j], cot_r.at[j])
        c = cot_all[j]
        dh = dot_last(c, mean_out[...]) + dot_last(c * s_out.astype(BF), pert_out[...]) * s_hid
        d = (dh * slope).astype(BF)
        df = d * s_mid.astype(BF)
        dpre[j] = d
        dpre_f[j] = df
        dn = (dot_last(d, mean_in[...]) + dot_last(df, pert_in[...]) * s_in).astype(BF)
        if first:
            own[1] = dn
        else:
            part_d[(k - 1) % slots] = dn
            dnr_copy(k, j).start()

    block(0, True)

    def step(k, carry):
        block(k, False)
        return carry

    lax.fori_loop(1, seq, step, 0)

    rows = seq * patches

    def produce(a, left, right):
        total_rows, cols = left.shape[2], right.shape[2]
        _, _, pr, pc = pieces[a].shape
        tile = min(256, total_rows)
        rhs = right[...].reshape(rows, cols)
        for t in range(total_rows // tile):
            lhs = left[:, :, t * tile : (t + 1) * tile].reshape(rows, tile)
            g = dot_first(lhs, rhs).astype(BF)
            for c in range(CORES):
                for s in range(nz):
                    lo = (c * nz + s) * pr if pc == cols else s * pr
                    left_col = 0 if pc == cols else c * pc
                    if t * tile <= lo < (t + 1) * tile:
                        pieces[a][c, s] = g[lo - t * tile : lo - t * tile + pr, left_col : left_col + pc]
        pair_copy(a).start()

    def pair_copy(a):
        return remote(pieces[a].at[1 - core], pairs[a], pair_s.at[a], pair_r.at[a], partner)

    def up_copy(a, d, src):
        return remote(src, ups[a].at[d], up_s.at[a, d], up_r.at[a, d], above)

    def down_copy(a, d, src):
        return remote(src, downs[a].at[d], dn_s.at[a, d], dn_r.at[a, d], below)

    def merge(a):
        arrived(pairs[a], pair_r.at[a])
        pairs[a][...] = (pairs[a][...].astype(F32) + pieces[a][core].astype(F32)).astype(BF)

        @pl.when(z == 0)
        def _():
            for d in range(nz - 1, 0, -1):
                up_copy(a, d, pairs[a].at[d]).start()

        @pl.when(z == nz - 1)
        def _():
            for d in range(nz - 1):
                down_copy(a, d, pairs[a].at[d]).start()

    def chain(a):
        for i in range(nz):
            d = nz - 1 - i

            @pl.when((z > 0) & (z < d))
            def _():
                arrived(ups[a].at[d], up_r.at[a, d])
                ups[a][d] = (ups[a][d].astype(F32) + pairs[a][d].astype(F32)).astype(BF)
                up_copy(a, d, ups[a].at[d]).start()

            @pl.when((z < nz - 1) & (z > i))
            def _():
                arrived(downs[a].at[i], dn_r.at[a, i])
                downs[a][i] = (downs[a][i].astype(F32) + pairs[a][i].astype(F32)).astype(BF)
                down_copy(a, i, downs[a].at[i]).start()

    def hand_up(a, d):
        return remote(fulls[a].at[core, d], fulls[a].at[core, d], gu_s.at[a, d], gu_r.at[a, d], above)

    def hand_down(a, d):
        return remote(fulls[a].at[core, d], fulls[a].at[core, d], gd_s.at[a, d], gd_r.at[a, d], below)

    def hand_over(a, d):
        return remote(fulls[a].at[core, d], fulls[a].at[core, d], gp_s.at[a, d], gp_r.at[a, d], partner)

    def finish(a):
        for d in range(nz):
            @pl.when(z == d)
            def _():
                total = pairs[a][d].astype(F32)
                if d > 0:
                    arrived(ups[a].at[d], up_r.at[a, d])
                    total = total + ups[a][d].astype(F32)
                if d < nz - 1:
                    arrived(downs[a].at[d], dn_r.at[a, d])
                    total = total + downs[a][d].astype(F32)
                fulls[a][core, d] = total.astype(BF)
                if d < nz - 1:
                    hand_up(a, d).start()
                if d > 0:
                    hand_down(a, d).start()
                hand_over(a, d).start()

    def spread(a):
        for i in range(1, nz):
            low, high = z - i, z + i

            @pl.when(low >= 0)
            def _():
                arrived(fulls[a].at[core, low], gu_r.at[a, low])

                @pl.when(z < nz - 1)
                def _():
                    hand_up(a, low).start()

                hand_over(a, low).start()

            @pl.when(high < nz)
            def _():
                arrived(fulls[a].at[core, high], gd_r.at[a, high])

                @pl.when(z > 0)
                def _():
                    hand_down(a, high).start()

                hand_over(a, high).start()

    produce(0, hid, cot_all)
    produce(2, nrm_all, dpre)
    merge(0)
    for k in range(1, seq):
        nrm_copy(k).wait_send()
    cot_all[...] = cot_all[...] * f_out[...].astype(F32).astype(BF)[:, None, :]
    produce(1, hid_f, cot_all)
    chain(0)
    merge(2)
    nrm_all[...] = nrm_all[...] * f_in[...].astype(F32).astype(BF)[:, None, :]
    produce(3, nrm_all, dpre_f)
    merge(1)
    merge(3)
    chain(2)
    finish(0)
    chain(1)
    finish(2)
    spread(0)
    chain(3)
    finish(1)
    spread(2)
    finish(3)
    spread(1)

    def gather_sum(slot, buf, sem):
        total = own[slot].astype(F32)
        for k in range(1, seq):
            j = shifted(k, -1)
            arrived(buf.at[j], sem.at[j])
            total = total + buf[j].astype(F32)
        return total

    resid_f = resid[...].astype(F32)
    out_block[0] = (resid_f + gather_sum(0, got_m, mix_r)).astype(BF)
    scaled = gather_sum(1, got_d, dnr_r) * gain_f
    ahat, rstd = norm_stats(resid_f)
    back = rstd * (
        scaled
        - jnp.mean(scaled, axis=-1, keepdims=True)
        - ahat * jnp.mean(scaled * ahat, axis=-1, keepdims=True)
    )
    out_grad[0] = (cot[0].astype(F32) + back).astype(BF)
    spread(3)

    outs = (o_mo, o_so, o_mi, o_si)

    def drain(a):
        for d in range(nz):
            arrived(fulls[a].at[1 - core, d], gp_r.at[a, d])
        pltpu.make_async_copy(fulls[a], outs[a], out_sem.at[a]).start()

    for a in range(4):
        drain(a)

    for k in range(1, seq):
        cot_copy(k).wait_send()
    for k in range(max(1, seq - slots), seq):
        mix_copy(k, me).wait_send()
        dnr_copy(k, me).wait_send()
    for a in range(4):
        pair_copy(a).wait_send()
        for d in range(nz):
            @pl.when((z < d) & (z < nz - 1))
            def _():
                up_copy(a, d, ups[a].at[d]).wait_send()

            @pl.when((z > d) & (z > 0))
            def _():
                down_copy(a, d, downs[a].at[d]).wait_send()

            @pl.when((z >= d) & (z < nz - 1))
            def _():
                hand_up(a, d).wait_send()

            @pl.when((z <= d) & (z > 0))
            def _():
                hand_down(a, d).wait_send()

            hand_over(a, d).wait_send()
    for a in range(4):
        pltpu.make_async_copy(fulls[a], outs[a], out_sem.at[a]).wait()


def body(dp, seq, *args):
    tokens, mean_in, mean_out = args[0], args[5], args[8]
    noise_in, noise_out = args[7], args[10]
    own, patches, width = tokens.shape
    assert own == 1
    hidden = mean_in.shape[1]
    nz = dp // CORES
    shapes = [(hidden, width)] * 2 + [(width, hidden)] * 2
    cut = [piece_shape(r, c, dp) for r, c in shapes]
    slots = max(1, min(seq - 1, 4))
    args = list(args)
    args[4] = args[4].reshape(1, width)
    vm = pltpu.VMEM
    tokens_all = (seq, patches, width)
    hidden_all = (seq, patches, hidden)
    dma = pltpu.SemaphoreType.DMA
    full = [(CORES, nz) + c for c in cut]
    scratch = [
        vm(mean_in.shape, BF),
        vm(mean_out.shape, BF),
        vm((patches, width), BF),
        vm(tokens_all, BF),
        vm(tokens_all, BF),
        *[vm(hidden_all, BF) for _ in range(4)],
        vm((2, patches, width), BF),
        vm((slots, patches, width), BF),
        vm((slots, patches, width), BF),
        vm(tokens_all, BF),
        vm(tokens_all, BF),
        [vm(f, BF) for f in full],
        *[[vm(f[1:], BF) for f in full] for _ in range(3)],
        [vm(f, BF) for f in full],
        *[dma((seq,)) for _ in range(4)],
        dma((slots,)), dma((seq,)), dma((slots,)), dma((seq,)),
        dma((4,)), dma((4,)),
        *[dma((4, nz)) for _ in range(10)],
        dma((4,)),
    ]
    whole = pl.BlockSpec(memory_space=pltpu.VMEM)
    away = pl.BlockSpec(memory_space=pl.ANY)
    res = pl.pallas_call(
        functools.partial(kernel, dp, seq),
        out_shape=[jax.ShapeDtypeStruct(tokens.shape, BF)] * 2
        + [jax.ShapeDtypeStruct(f, BF) for f in full],
        in_specs=[whole] * 16,
        out_specs=[whole, whole] + [away] * 4,
        scratch_shapes=scratch,
        compiler_params=pltpu.CompilerParams(
            collective_id=0, has_side_effects=True, vmem_limit_bytes=60 * 1024 * 1024
        ),
    )(*args)

    def assemble(a):
        r, c = shapes[a]
        g = res[2 + a]
        if cut[a][1] != c:
            g = jnp.transpose(g, (1, 2, 0, 3))
        return g.reshape(r, c).astype(F32)

    return (
        res[0],
        res[1],
        assemble(2),
        assemble(3) * noise_in.astype(F32),
        assemble(0),
        assemble(1) * noise_out.astype(F32),
    )


def solution(mesh):
    dp, seq = mesh.shape["dp"], mesh.shape["seq"]
    images = P(("dp", "seq"), None, None)
    cols, rows = P(None, "seq"), P("seq", None)
    return jax.shard_map(
        functools.partial(body, dp, seq),
        mesh=mesh,
        in_specs=(
            images, images, images, images, P(),
            cols, cols, cols, rows, rows, rows,
            P("dp", None), P("dp", "seq"), P("dp", "seq"), P("dp", None),
            images,
        ),
        out_specs=(images, images, cols, cols, rows, rows),
        check_vma=False,
    )
```

```python
import functools
import math

import jax
import jax.numpy as jnp
from jax import lax
from jax.experimental import pallas as pl
from jax.experimental.pallas import tpu as pltpu
from jax.sharding import PartitionSpec as P

HEADS = 16
LANES = 128
CORES = 2
BF = jnp.bfloat16
F32 = jnp.float32
MESH = pl.DeviceIdType.MESH


def piece_shape(rows, cols, dp):
    if (rows // dp) % 16 == 0:
        return rows // dp, cols
    return rows * CORES // dp, cols // CORES


def dot_last(left, right):
    return lax.dot_general(left, right, (((1,), (1,)), ((), ())), preferred_element_type=F32)


def dot_first(left, right):
    return lax.dot_general(left, right, (((0,), (0,)), ((), ())), preferred_element_type=F32)


def dot(left, right):
    return jnp.dot(left, right, preferred_element_type=F32)


def norm_stats(resid_f):
    centered = resid_f - jnp.mean(resid_f, axis=-1, keepdims=True)
    rstd = lax.rsqrt(jnp.mean(centered * centered, axis=-1, keepdims=True) + 1e-06)
    return centered * rstd, rstd


def kernel(
    dp,
    seq,
    tok, que, key, val, gain, h_mi, h_si, h_ni, h_mo, h_so, h_no,
    f_in, f_mid, f_hid, f_out, cot,
    out_block, out_grad, o_mo, o_so, o_mi, o_si,
    mean_in, sig_in, noi_in, mean_out, sig_out, noi_out,
    pert_in, pert_out, resid, cot_all, nrm_all, hid, hid_f, dpre, dpre_f,
    own, part_m, part_d, got_m, got_d,
    pieces, pairs, ups, downs, fulls,
    cot_s, cot_r, nrm_s, nrm_r, mix_s, mix_r, dnr_s, dnr_r,
    pair_s, pair_r, up_s, up_r, dn_s, dn_r, gu_s, gu_r, gd_s, gd_r, gp_s, gp_r, out_sem,
    cf_s, cf_r, nf_s, nf_r, load_sem,
):
    my_dp = lax.axis_index("dp")
    me = lax.axis_index("seq")
    nz = dp // CORES
    z = my_dp // CORES
    core = my_dp % CORES
    partner = (z * CORES + (1 - core), me)
    above = (my_dp + CORES, me)
    below = (my_dp - CORES, me)
    base = math.isqrt(seq)
    if base * base != seq:
        base = seq
    tall = seq // base
    slots = part_m.shape[0]
    patches, width = resid.shape
    head_dim = width // HEADS
    scale = head_dim ** (-0.5)

    square = seq == 4 and base == 2
    direct = (1, 2) if square else tuple(range(1, seq))
    half = patches // 2
    loads = [
        pltpu.make_async_copy(away, near, load_sem.at[i])
        for i, (away, near) in enumerate(
            zip((h_si, h_ni, h_so, h_no, h_mi, h_mo), (sig_in, noi_in, sig_out, noi_out, mean_in, mean_out))
        )
    ]
    for load in loads:
        load.start()

    def shifted(k, sign):
        row = (me // base + sign * (k // base) + tall) % tall
        return row * base + (me % base + sign * (k % base) + base) % base

    def remote(src, dst, s, r, dev):
        return pltpu.make_async_remote_copy(
            src_ref=src, dst_ref=dst, send_sem=s, recv_sem=r, device_id=dev, device_id_type=MESH
        )

    def peer(index):
        return (my_dp, index)

    barrier = pltpu.get_barrier_semaphore()

    def greet(dev):
        pl.semaphore_signal(barrier, inc=1, device_id=dev, device_id_type=MESH)

    for k in range(1, seq):
        greet(peer(shifted(k, 1)))
    greet(partner)

    @pl.when(z > 0)
    def _():
        greet(below)

    @pl.when(z < nz - 1)
    def _():
        greet(above)

    chained = (z + nz - 1) // nz + (nz - 1 - z + nz - 1) // nz
    pl.semaphore_wait(barrier, seq + chained)

    def cot_copy(k):
        return remote(cot.at[0], cot_all.at[me], cot_s.at[k], cot_r.at[me], peer(shifted(k, 1)))

    def nrm_copy(k):
        return remote(
            nrm_all.at[me], nrm_all.at[me], nrm_s.at[k], nrm_r.at[me], peer(shifted(k, 1))
        )

    def relay(buf, k, s, r):
        part = buf.at[shifted(k, -1), pl.ds((k - 1) * half, half)]
        return remote(part, part, s.at[k - 1], r.at[k - 1], peer(shifted(3 - k, 1)))

    def relayed(buf, j, r):
        for i in range(2):
            arrived(buf.at[j, pl.ds(i * half, half)], r.at[i])

    def arrived(dst, sem):
        remote(dst, dst, sem, sem, peer(me)).wait_recv()

    for k in direct:
        cot_copy(k).start()

    group = LANES // head_dim
    lane = lax.broadcasted_iota(jnp.int32, (1, LANES), 1)
    masks = [
        jnp.where((lane >= h * head_dim) & (lane < (h + 1) * head_dim), 1.0, 0.0).astype(F32)
        for h in range(group)
    ]

    def heads(p, carry):
        cols = pl.ds(pl.multiple_of(p * LANES, LANES), LANES)
        q, kk, v = que[0, :, cols], key[0, :, cols], val[0, :, cols]
        acc = jnp.zeros((patches, LANES), F32)
        for mask in masks:
            scores = dot_last(q * mask.astype(BF), kk) * scale
            expd = jnp.exp(scores - jnp.max(scores, axis=-1, keepdims=True))
            total = jnp.sum(expd, axis=-1, keepdims=True)
            acc = acc + (dot(expd.astype(BF), v) / total) * mask
        attn = acc.astype(BF).astype(F32)
        resid[:, cols] = (tok[0, :, cols].astype(F32) + attn).astype(BF)
        return carry

    lax.fori_loop(0, width // LANES, heads, 0)
    gain_f = gain[...].astype(F32)
    ahat, _ = norm_stats(resid[...].astype(F32))
    nrm_all[me] = (ahat * gain_f).astype(BF)
    for k in direct:
        nrm_copy(k).start()
    for load in loads:
        load.wait()

    pert_in[...] = (sig_in[...].astype(F32) * noi_in[...].astype(F32)).astype(BF)
    pert_out[...] = (sig_out[...].astype(F32) * noi_out[...].astype(F32)).astype(BF)
    cot_all[me] = cot[0]
    if square:
        for k in direct:
            j = shifted(k, -1)
            arrived(cot_all.at[j], cot_r.at[j])
            relay(cot_all, k, cf_s, cf_r).start()

    def mix_copy(k, j):
        slot = (k - 1) % slots
        return remote(part_m.at[slot], got_m.at[me], mix_s.at[slot], mix_r.at[me], peer(j))

    def dnr_copy(k, j):
        slot = (k - 1) % slots
        return remote(part_d.at[slot], got_d.at[me], dnr_s.at[slot], dnr_r.at[me], peer(j))

    def signs(ref, j):
        return ref[pl.ds(j, 1), :].astype(F32)

    def block(k, first):
        j = me if first else shifted(k, -1)
        s_in, s_mid, s_hid, s_out = signs(f_in, j), signs(f_mid, j), signs(f_hid, j), signs(f_out, j)
        if square and not first:
            @pl.when(k < 3)
            def _():
                arrived(nrm_all.at[j], nrm_r.at[j])
                relay(nrm_all, k, nf_s, nf_r).start()

            @pl.when(k == 3)
            def _():
                relayed(nrm_all, j, nf_r)
        elif not first:
            arrived(nrm_all.at[j], nrm_r.at[j])
        x = nrm_all[j]
        pre = dot(x, mean_in[...]) + dot(x * s_in.astype(BF), pert_in[...]) * s_mid
        cdf = 0.5 * (1.0 + lax.erf(pre * 0.7071067811865476))
        slope = cdf + pre * (jnp.exp(-0.5 * pre * pre) * 0.3989422804014327)
        h = (pre * cdf).astype(BF)
        hf = h * s_hid.astype(BF)
        hid[j] = h
        hid_f[j] = hf
        mixed = (dot(h, mean_out[...]) + dot(hf, pert_out[...]) * s_out).astype(BF)
        if first:
            own[0] = mixed
        else:
            @pl.when(k > slots)
            def _():
                mix_copy(k, j).wait_send()
                dnr_copy(k, j).wait_send()

            part_m[(k - 1) % slots] = mixed
            mix_copy(k, j).start()
            if square:
                @pl.when(k == 3)
                def _():
                    relayed(cot_all, j, cf_r)
            else:
                arrived(cot_all.at[j], cot_r.at[j])
        c = cot_all[j]
        dh = dot_last(c, mean_out[...]) + dot_last(c * s_out.astype(BF), pert_out[...]) * s_hid
        d = (dh * slope).astype(BF)
        df = d * s_mid.astype(BF)
        dpre[j] = d
        dpre_f[j] = df
        dn = (dot_last(d, mean_in[...]) + dot_last(df, pert_in[...]) * s_in).astype(BF)
        if first:
            own[1] = dn
        else:
            part_d[(k - 1) % slots] = dn
            dnr_copy(k, j).start()

    block(0, True)

    def step(k, carry):
        block(k, False)
        return carry

    lax.fori_loop(1, seq, step, 0)

    rows = seq * patches

    def produce(a, left, right):
        total_rows, cols = left.shape[2], right.shape[2]
        _, _, pr, pc = pieces[a].shape
        tile = min(256, total_rows)
        rhs = right[...].reshape(rows, cols)
        for t in range(total_rows // tile):
            lhs = left[:, :, t * tile : (t + 1) * tile].reshape(rows, tile)
            g = dot_first(lhs, rhs).astype(BF)
            for c in range(CORES):
                for s in range(nz):
                    lo = (c * nz + s) * pr if pc == cols else s * pr
                    left_col = 0 if pc == cols else c * pc
                    if t * tile <= lo < (t + 1) * tile:
                        pieces[a][c, s] = g[lo - t * tile : lo - t * tile + pr, left_col : left_col + pc]
        pair_copy(a).start()

    def pair_copy(a):
        return remote(pieces[a].at[1 - core], pairs[a], pair_s.at[a], pair_r.at[a], partner)

    def up_copy(a, d, src):
        return remote(src, ups[a].at[d], up_s.at[a, d], up_r.at[a, d], above)

    def down_copy(a, d, src):
        return remote(src, downs[a].at[d], dn_s.at[a, d], dn_r.at[a, d], below)

    def merge(a):
        arrived(pairs[a], pair_r.at[a])
        pairs[a][...] = (pairs[a][...].astype(F32) + pieces[a][core].astype(F32)).astype(BF)

        @pl.when(z == 0)
        def _():
            for d in range(nz - 1, 0, -1):
                up_copy(a, d, pairs[a].at[d]).start()

        @pl.when(z == nz - 1)
        def _():
            for d in range(nz - 1):
                down_copy(a, d, pairs[a].at[d]).start()

    def chain(a):
        for i in range(nz):
            d = nz - 1 - i

            @pl.when((z > 0) & (z < d))
            def _():
                arrived(ups[a].at[d], up_r.at[a, d])
                ups[a][d] = (ups[a][d].astype(F32) + pairs[a][d].astype(F32)).astype(BF)
                up_copy(a, d, ups[a].at[d]).start()

            @pl.when((z < nz - 1) & (z > i))
            def _():
                arrived(downs[a].at[i], dn_r.at[a, i])
                downs[a][i] = (downs[a][i].astype(F32) + pairs[a][i].astype(F32)).astype(BF)
                down_copy(a, i, downs[a].at[i]).start()

    def hand_up(a, d):
        return remote(fulls[a].at[core, d], fulls[a].at[core, d], gu_s.at[a, d], gu_r.at[a, d], above)

    def hand_down(a, d):
        return remote(fulls[a].at[core, d], fulls[a].at[core, d], gd_s.at[a, d], gd_r.at[a, d], below)

    def hand_over(a, d):
        return remote(fulls[a].at[core, d], fulls[a].at[core, d], gp_s.at[a, d], gp_r.at[a, d], partner)

    def finish(a):
        for d in range(nz):
            @pl.when(z == d)
            def _():
                total = pairs[a][d].astype(F32)
                if d > 0:
                    arrived(ups[a].at[d], up_r.at[a, d])
                    total = total + ups[a][d].astype(F32)
                if d < nz - 1:
                    arrived(downs[a].at[d], dn_r.at[a, d])
                    total = total + downs[a][d].astype(F32)
                fulls[a][core, d] = total.astype(BF)
                if d < nz - 1:
                    hand_up(a, d).start()
                if d > 0:
                    hand_down(a, d).start()
                hand_over(a, d).start()

    def spread(a):
        for i in range(1, nz):
            low, high = z - i, z + i

            @pl.when(low >= 0)
            def _():
                arrived(fulls[a].at[core, low], gu_r.at[a, low])

                @pl.when(z < nz - 1)
                def _():
                    hand_up(a, low).start()

                hand_over(a, low).start()

            @pl.when(high < nz)
            def _():
                arrived(fulls[a].at[core, high], gd_r.at[a, high])

                @pl.when(z > 0)
                def _():
                    hand_down(a, high).start()

                hand_over(a, high).start()

    produce(0, hid, cot_all)
    produce(2, nrm_all, dpre)
    merge(0)
    for k in direct:
        nrm_copy(k).wait_send()
        if square:
            relay(nrm_all, k, nf_s, nf_r).wait_send()
            relay(cot_all, k, cf_s, cf_r).wait_send()
    cot_all[...] = cot_all[...] * f_out[...].astype(F32).astype(BF)[:, None, :]
    produce(1, hid_f, cot_all)
    chain(0)
    merge(2)
    nrm_all[...] = nrm_all[...] * f_in[...].astype(F32).astype(BF)[:, None, :]
    produce(3, nrm_all, dpre_f)
    merge(1)
    merge(3)
    chain(2)
    finish(0)
    chain(1)
    finish(2)
    spread(0)
    chain(3)
    finish(1)
    spread(2)
    finish(3)
    spread(1)

    def gather_sum(slot, buf, sem):
        total = own[slot].astype(F32)
        for k in range(1, seq):
            j = shifted(k, -1)
            arrived(buf.at[j], sem.at[j])
            total = total + buf[j].astype(F32)
        return total

    resid_f = resid[...].astype(F32)
    out_block[0] = (resid_f + gather_sum(0, got_m, mix_r)).astype(BF)
    scaled = gather_sum(1, got_d, dnr_r) * gain_f
    ahat, rstd = norm_stats(resid_f)
    back = rstd * (
        scaled
        - jnp.mean(scaled, axis=-1, keepdims=True)
        - ahat * jnp.mean(scaled * ahat, axis=-1, keepdims=True)
    )
    out_grad[0] = (cot[0].astype(F32) + back).astype(BF)
    spread(3)

    outs = (o_mo, o_so, o_mi, o_si)

    def drain(a):
        for d in range(nz):
            arrived(fulls[a].at[1 - core, d], gp_r.at[a, d])
        pltpu.make_async_copy(fulls[a], outs[a], out_sem.at[a]).start()

    for a in range(4):
        drain(a)

    for k in direct:
        cot_copy(k).wait_send()
    for k in range(max(1, seq - slots), seq):
        mix_copy(k, me).wait_send()
        dnr_copy(k, me).wait_send()
    for a in range(4):
        pair_copy(a).wait_send()
        for d in range(nz):
            @pl.when((z < d) & (z < nz - 1))
            def _():
                up_copy(a, d, ups[a].at[d]).wait_send()

            @pl.when((z > d) & (z > 0))
            def _():
                down_copy(a, d, downs[a].at[d]).wait_send()

            @pl.when((z >= d) & (z < nz - 1))
            def _():
                hand_up(a, d).wait_send()

            @pl.when((z <= d) & (z > 0))
            def _():
                hand_down(a, d).wait_send()

            hand_over(a, d).wait_send()
    for a in range(4):
        pltpu.make_async_copy(fulls[a], outs[a], out_sem.at[a]).wait()


def body(dp, seq, *args):
    tokens, mean_in, mean_out = args[0], args[5], args[8]
    noise_in, noise_out = args[7], args[10]
    own, patches, width = tokens.shape
    assert own == 1
    hidden = mean_in.shape[1]
    nz = dp // CORES
    shapes = [(hidden, width)] * 2 + [(width, hidden)] * 2
    cut = [piece_shape(r, c, dp) for r, c in shapes]
    slots = max(1, min(seq - 1, 4))
    args = list(args)
    args[4] = args[4].reshape(1, width)
    vm = pltpu.VMEM
    tokens_all = (seq, patches, width)
    hidden_all = (seq, patches, hidden)
    dma = pltpu.SemaphoreType.DMA
    full = [(CORES, nz) + c for c in cut]
    scratch = [
        *[vm(a.shape, BF) for a in args[5:11]],
        vm(mean_in.shape, BF),
        vm(mean_out.shape, BF),
        vm((patches, width), BF),
        vm(tokens_all, BF),
        vm(tokens_all, BF),
        *[vm(hidden_all, BF) for _ in range(4)],
        vm((2, patches, width), BF),
        vm((slots, patches, width), BF),
        vm((slots, patches, width), BF),
        vm(tokens_all, BF),
        vm(tokens_all, BF),
        [vm(f, BF) for f in full],
        *[[vm(f[1:], BF) for f in full] for _ in range(3)],
        [vm(f, BF) for f in full],
        *[dma((seq,)) for _ in range(4)],
        dma((slots,)), dma((seq,)), dma((slots,)), dma((seq,)),
        dma((4,)), dma((4,)),
        *[dma((4, nz)) for _ in range(10)],
        dma((4,)),
        *[dma((2,)) for _ in range(4)],
        dma((6,)),
    ]
    whole = pl.BlockSpec(memory_space=pltpu.VMEM)
    away = pl.BlockSpec(memory_space=pl.ANY)
    res = pl.pallas_call(
        functools.partial(kernel, dp, seq),
        out_shape=[jax.ShapeDtypeStruct(tokens.shape, BF)] * 2
        + [jax.ShapeDtypeStruct(f, BF) for f in full],
        in_specs=[whole] * 5 + [away] * 6 + [whole] * 5,
        out_specs=[whole, whole] + [away] * 4,
        scratch_shapes=scratch,
        compiler_params=pltpu.CompilerParams(
            collective_id=0, has_side_effects=True, vmem_limit_bytes=60 * 1024 * 1024
        ),
    )(*args)

    def assemble(a):
        r, c = shapes[a]
        g = res[2 + a]
        if cut[a][1] != c:
            g = jnp.transpose(g, (1, 2, 0, 3))
        return g.reshape(r, c).astype(F32)

    return (
        res[0],
        res[1],
        assemble(2),
        assemble(3) * noise_in.astype(F32),
        assemble(0),
        assemble(1) * noise_out.astype(F32),
    )


def solution(mesh):
    dp, seq = mesh.shape["dp"], mesh.shape["seq"]
    images = P(("dp", "seq"), None, None)
    cols, rows = P(None, "seq"), P("seq", None)
    return jax.shard_map(
        functools.partial(body, dp, seq),
        mesh=mesh,
        in_specs=(
            images, images, images, images, P(),
            cols, cols, cols, rows, rows, rows,
            P("dp", None), P("dp", "seq"), P("dp", "seq"), P("dp", None),
            images,
        ),
        out_specs=(images, images, cols, cols, rows, rows),
        check_vma=False,
    )
```
